256 devices in a mesh: row: 8 (over x_hi, y), col: 32 (over x_lo, z, core).
Axes of the slice: x: 4 (x_hi: 2, x_lo: 2; x = x_hi * 2 + x_lo), y: 4, z: 8, core: 2. Of those that a mesh axis runs over, the one named last changes fastest.
Arguments:
- out_grad: bfloat16 [32768, 512], P('col', 'row'), may hold values from -6 to 6
- node_in: bfloat16 [32768, 512], P(('row', 'col')), may hold values from -0.03125 to 0.03125
- weights: bfloat16 [3, 512, 512], replicated, may hold values from -0.25 to 0.25
- tile_vals: bfloat16 [3, 32, 8, 32, 128, 128], P(None, 'col', 'row'), may hold values from -0.15625 to 0.15625
- tile_rows: int32 [3, 32, 8, 32], P(None, 'col', 'row'), may hold values from 0 to 7
- tile_cols: int32 [3, 32, 8, 32], P(None, 'col', 'row'), may hold values from 0 to 31
- tile_count: int32 [3, 32, 8], P(None, 'col', 'row'), may hold values from 1 to 32, as said below
Outputs:
- d_nodes: bfloat16 [32768, 512], P(('row', 'col'))
- d_weights: float32 [3, 512, 512], replicated
The draws below stay inside these ranges and needn't reach their ends.
Inputs may be any that keep to these rules, and one draw needn't show every extreme that they name: Only the first tile_count slots of a block's list hold tiles; later slots are ignored. In every relation some block uses all 32 slots. `tile_rows`: coordinates may repeat within a block's list; such tiles add.
All inputs are finite; a program needn't handle non-finite values.
Results may differ from the reference program's by a relative error of at most 0.005.
Values may be sent and summed in bfloat16 or wider, within the bound.
A program may use at most 256 MiB of HBM per device.

```python
import jax
import jax.numpy as jnp
from jax import lax

D = 512
R = 3
TILE = 128
N_DEV = 128
CAP = 32
ROW_GROUPS = 8
COL_GROUPS = 32
NODES = 32768
TR = 8
TC = 32


def draw_tile_count(key, part):
    grid_shape = (R, COL_GROUPS, ROW_GROUPS)
    levels = jax.random.randint(jax.random.fold_in(key, 11), grid_shape, 1, 9)
    counts = jnp.maximum(1, CAP * levels * levels // 64)
    full_device = jax.random.randint(jax.random.fold_in(key, 12), (R,), 0, COL_GROUPS * ROW_GROUPS)
    flat_counts = counts.reshape(R, COL_GROUPS * ROW_GROUPS)
    chosen = jnp.arange(COL_GROUPS * ROW_GROUPS)[None, :] == full_device[:, None]
    flat_counts = jnp.where(chosen, CAP, flat_counts)
    return flat_counts.reshape(grid_shape).astype(jnp.int32)


def touch_ends(array, own_key, least, largest):
    extent = array.shape
    place = [jax.random.randint(jax.random.fold_in(own_key, axis), (), 0, extent[axis]) for axis in range(len(extent))]
    array = array.at[tuple(place)].set(least)
    longest = extent.index(max(extent))
    place[longest] = (place[longest] + 1) % extent[longest]
    return array.at[tuple(place)].set(largest)


def shard_levels(rng, shape, cuts, low, largest):
    def one(position, blocks):
        draws = jax.random.uniform(jax.random.fold_in(jax.random.fold_in(rng, 6), position), (blocks,), jnp.float32, low / len(cuts), largest / len(cuts))
        return jnp.repeat(jnp.exp(draws), shape[position] // blocks).reshape((-1,) + (1,) * (len(shape) - position - 1))

    loudness = one(*cuts[0])
    for cut in cuts[1:]:
        loudness = loudness * one(*cut)
    return loudness


def bell_draw(stream_key, dims, spread, most, split=(), held_as=jnp.bfloat16):
    drawn = spread * jax.random.normal(stream_key, dims, jnp.float32)
    if split:
        drawn = drawn * shard_levels(stream_key, dims, split, -0.22, 0.18)
    return jnp.clip(drawn, -most, most).astype(held_as)


def setup_inputs(seed: int = 0) -> dict:
    streams_of = jax.random.split(jax.random.key(seed), 8)
    out_grad = bell_draw(streams_of[0], (NODES, D), 1.0, 6.0, ((0, 32), (1, 8)))
    node_in = bell_draw(streams_of[1], (NODES, D), NODES ** -0.5, 0.03125, ((0, 256),))
    weights = bell_draw(streams_of[2], (R, D, D), D ** -0.5, 0.25)
    tile_vals = bell_draw(streams_of[3], (R, COL_GROUPS, ROW_GROUPS, CAP, TILE, TILE), (CAP * COL_GROUPS * 2 * TILE // (5 * TC)) ** -0.5, 0.15625, ((1, 32), (2, 8)))
    tile_rows = touch_ends(jax.random.randint(streams_of[4], (R, COL_GROUPS, ROW_GROUPS, CAP), 0, TR), jax.random.fold_in(streams_of[4], 1), 0, TR - 1).astype(jnp.int32)
    tile_cols = touch_ends(jax.random.randint(streams_of[5], (R, COL_GROUPS, ROW_GROUPS, CAP), 0, TC), jax.random.fold_in(streams_of[5], 1), 0, TC - 1).astype(jnp.int32)
    tile_count = draw_tile_count(jax.random.fold_in(streams_of[7], 71), 0)
    return {"out_grad": out_grad, "node_in": node_in, "weights": weights, "tile_vals": tile_vals, "tile_rows": tile_rows, "tile_cols": tile_cols, "tile_count": tile_count}


def block_products(operand, tile_block, row_ids, col_ids, count_now, block_index):
    group_col = block_index // ROW_GROUPS
    group_row = block_index % ROW_GROUPS
    lanes = jnp.arange(TILE, dtype=jnp.int32)
    source_ids = (group_col * (N_DEV * ROW_GROUPS) + row_ids[:, None] * TILE + lanes[None, :]).astype(jnp.int32)
    sources = jnp.take(operand, source_ids.reshape(-1), axis=0).reshape(CAP, TILE, 2 * D)
    live = (jnp.arange(CAP, dtype=jnp.int32) < count_now).astype(jnp.float32)
    products = jnp.einsum("skt,skd->std", tile_block.astype(jnp.float32), sources.astype(jnp.float32), precision=lax.Precision.HIGHEST)
    products = products * live[:, None, None]
    target_ids = (group_row * (N_DEV * COL_GROUPS) + col_ids[:, None] * TILE + lanes[None, :]).astype(jnp.int32)
    return target_ids.reshape(-1), products.reshape(CAP * TILE, 2 * D)


def reference(out_grad, node_in, weights, tile_vals, tile_rows, tile_cols, tile_count):
    blocks = COL_GROUPS * ROW_GROUPS
    block_ids = jnp.arange(blocks, dtype=jnp.int32)
    mixed_total = jnp.zeros((NODES, D), jnp.float32)
    weight_grads = []
    inputs_wide = node_in.astype(jnp.float32)
    for relation in range(R):
        premixed = jnp.dot(out_grad, weights[relation].T, preferred_element_type=jnp.float32).astype(jnp.bfloat16)
        operand = jnp.concatenate([out_grad, premixed], axis=1)

        def block_step(summed, inputs):
            target_ids, products = block_products(operand, inputs[0], inputs[1], inputs[2], inputs[3], inputs[4])
            return summed.at[target_ids].add(products), None

        scanned = (tile_vals[relation].reshape(blocks, CAP, TILE, TILE), tile_rows[relation].reshape(blocks, CAP), tile_cols[relation].reshape(blocks, CAP), tile_count[relation].reshape(blocks), block_ids)
        start_sums = jnp.zeros((NODES, 2 * D), jnp.float32)
        summed, ignored = lax.scan(block_step, start_sums, scanned)
        weight_grads.append(jnp.dot(inputs_wide.T, summed[:, :D], precision=lax.Precision.HIGHEST))
        mixed_total = mixed_total + summed[:, D:]
    return mixed_total.astype(jnp.bfloat16), jnp.stack(weight_grads)
```

```python
import functools

import jax
import jax.numpy as jnp
from jax import lax
from jax.experimental import pallas as pl
from jax.experimental.pallas import tpu as pltpu
from jax.sharding import PartitionSpec as P

MESH = pl.DeviceIdType.MESH
F32 = jnp.float32
BF16 = jnp.bfloat16
SEMS = 360


def main_kernel(
    nr, nc, relations, cap,
    gin_ref, nodes_ref, rows_s, cols_s, count_s, rows_v, cols_v, w_hbm, t_hbm,
    dn_ref, ag_ref,
    gt, gy, w, tiles, tilest, xall, pm, acc, nsend, nrecv, nown, meta, link,
    zsa, zra, zsb, zrb, xs, xr, xf, dwrecv, pbuf, precv, zbuf, zrecv,
    load_sem, ssem, rsem,
):
    ny = nr // 2
    nz = nc // 4
    nk = nc // 2
    nd, f = nodes_ref.shape
    gb, tn = gin_ref.shape
    nt = tn // nd
    half = f // 2
    hb = half // nd
    me_r = lax.axis_index("row")
    me_c = lax.axis_index("col")
    xh = me_r // ny
    y = lax.rem(me_r, ny)
    xl = me_c // (2 * nz)
    z = lax.rem(me_c // 2, nz)
    core = lax.rem(me_c, 2)
    other = 1 - core

    def zat(dz):
        return lax.rem(z + (dz + 2 * nz), nz)

    def kat(x, zz):
        return x * nz + zz

    def cat(x, zz):
        return kat(x, zz) * 2 + core

    sibling = {"col": kat(xl, z) * 2 + other}
    xdev = {"col": cat(1 - xl, z)}
    xhdev = {"row": (1 - xh) * ny + y}

    def zdev(dz):
        return {"col": cat(xl, zat(dz))}

    def yat(dy):
        return lax.rem(y + (dy + 2 * ny), ny)

    def ydev(dy):
        return {"row": xh * ny + yat(dy)}

    def row_peer(d):
        r = lax.rem(me_r + d, nr)
        side = lax.rem(xl + xh + r // ny, 2)
        return {"row": r, "col": cat(side, z)}

    def k_peer(d):
        k = lax.rem(kat(xl, z) + d, nk)
        return k, {"col": k * 2 + core}

    used = [0]
    started = []

    def send(src, dst, dev):
        i = used[0]
        used[0] += 1
        c = pltpu.make_async_remote_copy(
            src_ref=src, dst_ref=dst, send_sem=ssem.at[i], recv_sem=rsem.at[i],
            device_id=dev, device_id_type=MESH,
        )
        c.start()
        started.append(c)
        return c

    load_w = pltpu.make_async_copy(w_hbm, w, load_sem.at[0])
    load_t = pltpu.make_async_copy(t_hbm, tiles, load_sem.at[1])
    load_t.start()
    load_w.start()

    barrier = pltpu.get_barrier_semaphore()
    for d in range(1, nr):
        pl.semaphore_signal(barrier, inc=1, device_id=row_peer(d), device_id_type=MESH)
    for d in range(1, nk):
        pl.semaphore_signal(barrier, inc=1, device_id=k_peer(d)[1], device_id_type=MESH)
    pl.semaphore_signal(barrier, inc=1, device_id=sibling, device_id_type=MESH)
    pl.semaphore_signal(barrier, inc=1, device_id=xhdev, device_id_type=MESH)
    pl.semaphore_wait(barrier, nr - 1 + nk - 1 + 2)

    def hops(n, orient, way):
        return n // 2 if way == orient else n - 1 - n // 2

    gh = gb // 2
    g_streams = {"o0": (0, 1), "o1": (1, -1), "p0": (0, 1), "p1": (1, -1)}

    def g_ref(st, dy):
        side = xh if st[0] == "o" else 1 - xh
        row = (side * ny + yat(dy)) * gb + g_streams[st][0] * gh
        return gt.at[pl.ds(pl.multiple_of(row, gh), gh), :]

    gcopy = {}

    def g_send(st, way, h):
        here = g_ref(st, -way * (h - 1))
        src = gin_ref.at[pl.ds(g_streams[st][0] * gh, gh), :] if h == 1 and st[0] == "o" else here
        gcopy[st, way, h] = send(src, here, ydev(way))

    def g_first(st):
        for way in (1, -1):
            if hops(ny, g_streams[st][1], way) >= 1:
                g_send(st, way, 1)

    def g_arrive(st, way, h):
        if (st, way, h) not in gcopy:
            return
        gcopy[st, way, h].wait_recv()
        if h < hops(ny, g_streams[st][1], way):
            g_send(st, way, h + 1)

    q = nd // 4
    x_streams = {"b0": (2 * q, q, 1), "b1": (3 * q, q, -1), "own": (0, 2 * q, 1), "par": (0, 2 * q, -1)}

    def x_rows(st):
        return slice(x_streams[st][0], x_streams[st][0] + x_streams[st][1])

    def x_ref(st, dz, x=None):
        if x is None:
            x = 1 - xl if st == "par" else xl
        return xall.at[cat(x, zat(dz)), x_rows(st), :]

    xcopy = {}
    xfwd = {}
    sib = []

    def to_sibling(ref):
        sib.append(send(ref, ref, sibling))

    def x_send(st, way, h):
        here = x_ref(st, -way * (h - 1))
        src = nodes_ref.at[x_rows(st), :] if h == 1 and st != "par" else here
        xcopy[st, way, h] = send(src, here, zdev(way))

    def x_first(st):
        for way in (1, -1):
            if hops(nz, x_streams[st][2], way) >= 1:
                x_send(st, way, 1)

    def x_arrive(st, way, h):
        if (st, way, h) not in xcopy:
            return
        xcopy[st, way, h].wait_recv()
        if h < hops(nz, x_streams[st][2], way):
            x_send(st, way, h + 1)
        here = x_ref(st, -way * h)
        if st[0] == "b":
            xfwd[st, way, h] = send(here, here, xdev)
        to_sibling(here)

    def x_cross(st, way, h):
        if (st, way, h) not in xfwd:
            return
        xfwd[st, way, h].wait_recv()
        to_sibling(x_ref(st, -way * h, 1 - xl))

    mine = xall.at[me_c]
    swap = send(nodes_ref.at[x_rows("par"), :], mine.at[x_rows("par"), :], xdev)
    for st in ("o0", "o1"):
        g_first(st)
    gswap = send(gin_ref, gt.at[pl.ds(pl.multiple_of(me_r * gb, gb), gb), :], xhdev)
    for st in ("b0", "b1", "own"):
        x_first(st)
    for st in ("b0", "b1"):
        xfwd[st, 0, 0] = send(nodes_ref.at[x_rows(st), :], mine.at[x_rows(st), :], xdev)
    sib.append(send(nodes_ref, mine, sibling))
    xall[me_c] = nodes_ref[...]
    gt[pl.ds(pl.multiple_of(me_r * gb, gb), gb), :] = gin_ref[...]

    slot_row = lax.broadcasted_iota(jnp.int32, (cap, cap), 0)
    slot_col = lax.broadcasted_iota(jnp.int32, (cap, cap), 1)
    places = lax.broadcasted_iota(jnp.int32, (cap, nc), 1)
    numbers = lax.broadcasted_iota(jnp.int32, (cap, nc), 0)

    def keys(ref, r):
        lane = lax.broadcasted_iota(jnp.int32, (1, cap), 1)
        key = jnp.where(lane < count_s[r], ref[r, 0], -1)
        turned = jnp.max(jnp.where(slot_row == slot_col, jnp.broadcast_to(key, (cap, cap)), -1), axis=1, keepdims=True)
        return key, turned

    def before(turned, key, offset, whole):
        same = turned == key
        if not whole:
            same = same & (slot_row < slot_col)
        return jnp.max(jnp.where(same, slot_row + (1 + offset), 0), axis=0, keepdims=True)

    def final(turned, offset):
        return jnp.max(jnp.where(turned == places, numbers + (1 + offset), 0), axis=0, keepdims=True)

    by_col = [keys(cols_v, r) for r in range(relations)]
    ends = final(by_col[0][1], 0)
    for r in range(1, relations):
        ends = jnp.maximum(ends, final(by_col[r][1], r * cap))
    meta[relations : relations + 1, 0:nc] = ends
    for r in range(relations):
        prior = before(by_col[r][1], by_col[r][0], r * cap, False)
        for e in range(r):
            prior = jnp.maximum(prior, before(by_col[e][1], by_col[r][0], e * cap, True))
        meta[r : r + 1, 0:cap] = prior
        key, turned = keys(rows_v, r)
        meta[4 + r : 5 + r, 0:cap] = before(turned, key, 0, False)
        meta[8 + r : 9 + r, 0:nc] = final(turned, 0)
    to_scalar = pltpu.make_async_copy(meta, link, load_sem.at[2])
    to_scalar.start()

    load_t.wait()

    def turn(r):
        def one(s, carry):
            tilest[r * cap + s] = tiles[r * cap + s].T
            return carry

        lax.fori_loop(0, cap, one, 0, unroll=4)

    turn(0)
    swap.wait_recv()
    to_sibling(x_ref("par", 0))
    x_first("par")
    gswap.wait_recv()
    for st in ("p0", "p1"):
        g_first(st)
    for way in (1, -1):
        for st in ("o0", "o1"):
            g_arrive(st, way, 1)
    turn(1)

    def x_round(h):
        for st in ("b0", "b1", "own", "par"):
            for way in (1, -1):
                x_arrive(st, way, h)
        for st in ("b0", "b1"):
            if h == 1:
                x_cross(st, 0, 0)
            for way in (1, -1):
                x_cross(st, way, h - 1)

    x_round(1)
    turn(2)
    for way in (1, -1):
        for st in ("p0", "p1"):
            g_arrive(st, way, 1)
    x_round(2)
    for h in range(2, ny):
        for way in (1, -1):
            for st in g_streams:
                g_arrive(st, way, h)
    load_w.wait()
    x_round(3)
    to_scalar.wait()

    for b in range(f // nd):
        gy[:, b * nd : (b + 1) * nd] = gt[b * nd : (b + 1) * nd, :].T
    for r in range(relations):
        prod = lax.dot_general(
            gy[...], w[r], (((1,), (1,)), ((), ())), preferred_element_type=F32
        ).astype(BF16)
        for i in range(nt):
            pm[r * nt + i] = prod[i * nd : (i + 1) * nd, :]
    acc[0] = jnp.zeros((nd, f), F32)

    def mix(r):
        def one(s, carry):
            t = r * cap + s
            p = jnp.dot(tilest[t], pm[r * nt + rows_s[r, 0, 0, s]], preferred_element_type=F32)
            acc[t + 1] = p + acc[link[r, s]]
            return carry

        lax.fori_loop(0, cap, one, 0, unroll=4)

    mix(0)
    mix(1)
    x_round(4)
    mix(2)

    order = [nz // 2]
    for d in range(nz // 2 - 1, 0, -1):
        order += [d, -d]
    order.append(0)
    ncore = {}
    for dz in order:
        for x in (0, 1):
            k = kat(1 - xl if x == 0 else xl, zat(dz))
            nsend[k] = acc[link[relations, 2 * k + other]]
            ncore[dz, x] = send(nsend.at[k], nrecv.at[k], sibling)

    xcross = {}

    def n_core(dz):
        for x in (0, 1):
            ncore[dz, x].wait_recv()
            k = kat(1 - xl if x == 0 else xl, zat(dz))
            nown[k] = nown[k] + nrecv[k]
        slot = zat(dz)
        xs[slot] = nown[kat(1 - xl, slot), 2 * q :, :].astype(BF16)
        xcross[dz] = send(xs.at[slot], xr.at[slot], xdev)

    def n_cross(dz):
        xcross[dz].wait_recv()
        k = kat(xl, zat(dz))
        nown[k, 2 * q :, :] = nown[k, 2 * q :, :] + xr[zat(dz)].astype(F32)

    zcopy = {}
    parts = {"par": (zsa, zra, 0), "own": (zsa, zra, 1), "b0": (zsb, zrb, 0), "b1": (zsb, zrb, 1)}

    def n_send(st, way, t):
        n = hops(nz, x_streams[st][2], way)
        if t > n:
            return
        sbuf, rbuf, slot = parts[st]
        side = 0 if way == 1 else 1
        x = 1 - xl if st == "par" else xl
        value = nown[kat(x, zat(way * (n + 1 - t))), x_rows(st), :]
        if t > 1:
            zcopy[st, way, t - 1].wait_recv()
            value = value + rbuf[slot, side, t - 2].astype(F32)
        sbuf[slot, side, t - 1] = value.astype(BF16)
        zcopy[st, way, t] = send(sbuf.at[slot, side, t - 1], rbuf.at[slot, side, t - 1], zdev(way))

    def n_final(st):
        x = 1 - xl if st == "par" else xl
        value = nown[kat(x, z), x_rows(st), :]
        for way in (1, -1):
            n = hops(nz, x_streams[st][2], way)
            if n:
                zcopy[st, way, n].wait_recv()
                _, rbuf, slot = parts[st]
                value = value + rbuf[slot, 0 if way == 1 else 1, n - 1].astype(F32)
        return value

    def n_round(t, names):
        for st in names:
            for way in (1, -1):
                n_send(st, way, t)

    base = cap + 1
    blocks = f // nd

    def terms(r):
        def one(s, carry):
            t = r * cap + s
            p = jnp.dot(tiles[t], xall[cols_s[r, 0, 0, s]], preferred_element_type=F32)
            acc[s + 1] = p + acc[link[4 + r, s]]
            return carry

        lax.fori_loop(0, cap, one, 0, unroll=4)
        for i in range(nt):
            gy[i * nd : (i + 1) * nd, :] = acc[link[8 + r, i]].astype(BF16)

    batches = {}

    def product(r):
        for b in range(blocks):
            acc[base + r * blocks + b] = jnp.dot(
                gt[b * nd : (b + 1) * nd, :], gy[...], preferred_element_type=F32
            )
        src = acc.at[pl.ds(base + r * blocks + other * hb, hb)]
        batches[0, r] = [send(src, dwrecv.at[r], sibling)]

    def arrived(stage, r):
        for c in batches[stage, r]:
            c.wait_recv()

    prow = f // nr

    def plane_scatter(r):
        arrived(0, r)
        for b in range(hb):
            total = acc[base + r * blocks + core * hb + b] + dwrecv[r, b]
            pbuf[r, :, b * nd : (b + 1) * nd] = total.astype(BF16).T
        copies = []
        for d in range(1, nr):
            peer = lax.rem(me_r + d, nr)
            src = pbuf.at[r, pl.ds(pl.multiple_of(peer * prow, prow), prow), :]
            copies.append(send(src, precv.at[r, d - 1], row_peer(d)))
        batches[1, r] = copies

    lanes = half // 128
    zrows = prow * lanes // nz

    def piece(zz):
        row = pl.multiple_of((zz // lanes) * zrows, zrows)
        lane = pl.multiple_of(lax.rem(zz, lanes) * 128, 128)
        return row, lane

    def z_scatter(r):
        arrived(1, r)
        part = pbuf[r, pl.ds(pl.multiple_of(me_r * prow, prow), prow), :].astype(F32)
        for d in range(1, nr):
            part = part + precv[r, d - 1].astype(F32)
        zbuf[r] = part.astype(BF16)
        me_k = kat(xl, z)
        row, lane = piece(z)
        zrecv[r, me_k] = zbuf[r, pl.ds(row, zrows), pl.ds(lane, 128)]
        copies = []
        for d in range(1, nk):
            k, dev = k_peer(d)
            row, lane = piece(lax.rem(k, nz))
            src = zbuf.at[r, pl.ds(row, zrows), pl.ds(lane, 128)]
            copies.append(send(src, zrecv.at[r, me_k], dev))
        batches[2, r] = copies

    def z_gather(r):
        arrived(2, r)
        final = zrecv[r, 0].astype(F32)
        for k in range(1, nk):
            final = final + zrecv[r, k].astype(F32)
        row, lane = piece(z)
        row = pl.multiple_of(r * f + me_r * prow + row, zrows)
        lane = pl.multiple_of(core * half + lane, 128)
        ag_ref[pl.ds(row, zrows), pl.ds(lane, 128)] = final.astype(BF16)
        mine = ag_ref.at[pl.ds(row, zrows), pl.ds(lane, 128)]
        batches[3, r] = [send(mine, mine, zdev(d)) for d in range(1, nz)]

    def strip(r, who):
        row = pl.multiple_of(r * f + who * prow, prow)
        return ag_ref.at[pl.ds(row, prow), pl.ds(pl.multiple_of(core * half, half), half)]

    last = []

    def plane_gather(r):
        arrived(3, r)
        mine = strip(r, me_r)
        batches[4, r] = [send(mine, mine, row_peer(d)) for d in range(1, nr)]
        last.append(send(mine, mine, sibling))

    def core_gather(r):
        for d in range(1, nr):
            batches[4, r][d - 1].wait_recv()
            there = strip(r, lax.rem(me_r + nr - d, nr))
            last.append(send(there, there, sibling))

    first = [d for d in order if abs(d) >= nz // 2 - 1]
    rest = [d for d in order if d not in first]
    a_names, b_names = ("par", "own"), ("b0", "b1")

    def keep(k, carry):
        nown[k] = acc[link[relations, 2 * k + core]]
        return carry

    lax.fori_loop(0, nk, keep, 0)
    for dz in first:
        n_core(dz)
    n_round(1, a_names)
    for h in range(5, nz + 1):
        x_round(h)
    for c in sib:
        c.wait_recv()
    terms(0)
    product(0)
    for dz in rest:
        n_core(dz)
    terms(1)
    product(1)
    plane_scatter(0)
    for dz in first:
        n_cross(dz)
    n_round(1, b_names)
    terms(2)
    product(2)
    plane_scatter(1)
    for dz in rest:
        n_cross(dz)
    plane_scatter(2)
    n_round(2, a_names)
    n_round(2, b_names)
    for r in range(relations):
        z_scatter(r)
    n_round(3, a_names)
    n_round(3, b_names)
    for r in range(relations):
        z_gather(r)
    for t in range(4, nz):
        n_round(t, a_names)
        n_round(t, b_names)
    for r in range(relations):
        plane_gather(r)
    xf[0] = n_final("par").astype(BF16)
    xlast = send(xf.at[0], xf.at[1], xdev)
    for st in b_names:
        dn_ref[x_rows(st), :] = n_final(st).astype(BF16)
    own = n_final("own")
    xlast.wait_recv()
    dn_ref[x_rows("own"), :] = (own + xf[1].astype(F32)).astype(BF16)
    for r in range(relations):
        core_gather(r)
    for c in last:
        c.wait_recv()
    for c in started:
        c.wait_send()
    assert used[0] <= SEMS


def widen_kernel(dn_ref, dw_ref, dn_out, dw_out, nodes, narrow, wide, in_sem, out_sem):
    parts, rows = narrow.shape[0], narrow.shape[1]

    def part(ref, k):
        return ref.at[k * rows : (k + 1) * rows, :]

    loads = [pltpu.make_async_copy(part(dw_ref, k), narrow.at[k], in_sem.at[k]) for k in range(parts)]
    stores = [pltpu.make_async_copy(wide.at[k], part(dw_out, k), out_sem.at[k]) for k in range(parts)]
    loads.append(pltpu.make_async_copy(dn_ref, nodes, in_sem.at[parts]))
    stores.append(pltpu.make_async_copy(nodes, dn_out, out_sem.at[parts]))
    for c in loads:
        c.start()
    for k in range(parts):
        loads[k].wait()
        wide[k] = narrow[k].astype(F32)
        stores[k].start()
    loads[parts].wait()
    stores[parts].start()
    for c in stores:
        c.wait()


def widen(d_nodes, gathered):
    total, f = gathered.shape
    parts = 6 if total % 96 == 0 else 1
    rows = total // parts
    hbm = pl.BlockSpec(memory_space=pltpu.HBM)
    return pl.pallas_call(
        widen_kernel,
        in_specs=[hbm, hbm],
        out_specs=(hbm, hbm),
        out_shape=(
            jax.ShapeDtypeStruct(d_nodes.shape, BF16),
            jax.ShapeDtypeStruct(gathered.shape, F32),
        ),
        scratch_shapes=[
            pltpu.VMEM(d_nodes.shape, BF16),
            pltpu.VMEM((parts, rows, f), BF16),
            pltpu.VMEM((parts, rows, f), F32),
            pltpu.SemaphoreType.DMA((parts + 1,)),
            pltpu.SemaphoreType.DMA((parts + 1,)),
        ],
    )(d_nodes, gathered)


def body(nr, nc, out_grad, node_in, weights, tile_vals, tile_rows, tile_cols, tile_count):
    relations, f = weights.shape[0], weights.shape[1]
    tn, width = out_grad.shape
    nd = node_in.shape[0]
    cap, tile = tile_vals.shape[3], tile_vals.shape[4]
    slots = relations * cap
    nt, nz, nk = tn // nd, nc // 4, nc // 2
    half = f // 2
    hb = half // nd
    prow = f // nr
    q = nd // 4
    hop = max(nz // 2, 1)
    zrows = prow * (half // 128) // nz

    dma = lambda *n: pltpu.SemaphoreType.DMA(n)
    vmem = pl.BlockSpec(memory_space=pltpu.VMEM)
    smem = pl.BlockSpec(memory_space=pltpu.SMEM)
    hbm = pl.BlockSpec(memory_space=pltpu.HBM)
    d_nodes, gathered = pl.pallas_call(
        functools.partial(main_kernel, nr, nc, relations, cap),
        out_shape=(
            jax.ShapeDtypeStruct((nd, f), BF16),
            jax.ShapeDtypeStruct((relations * f, f), BF16),
        ),
        in_specs=[vmem, vmem, smem, smem, smem, vmem, vmem, hbm, hbm],
        out_specs=(vmem, vmem),
        scratch_shapes=[
            pltpu.VMEM((f, tn), BF16),
            pltpu.VMEM((tn, f), BF16),
            pltpu.VMEM(weights.shape, BF16),
            pltpu.VMEM((slots, tile, tile), BF16),
            pltpu.VMEM((slots, tile, tile), BF16),
            pltpu.VMEM((nc, nd, f), BF16),
            pltpu.VMEM((relations * nt, nd, f), BF16),
            pltpu.VMEM((slots + 1, nd, f), F32),
            pltpu.VMEM((nk, nd, f), F32),
            pltpu.VMEM((nk, nd, f), F32),
            pltpu.VMEM((nk, nd, f), F32),
            pltpu.VMEM((16, 128), jnp.int32),
            pltpu.SMEM((16, 128), jnp.int32),
            pltpu.VMEM((2, 2, hop, 2 * q, f), BF16),
            pltpu.VMEM((2, 2, hop, 2 * q, f), BF16),
            pltpu.VMEM((2, 2, hop, q, f), BF16),
            pltpu.VMEM((2, 2, hop, q, f), BF16),
            pltpu.VMEM((nz, 2 * q, f), BF16),
            pltpu.VMEM((nz, 2 * q, f), BF16),
            pltpu.VMEM((2, 2 * q, f), BF16),
            pltpu.VMEM((relations, hb, nd, f), F32),
            pltpu.VMEM((relations, f, half), BF16),
            pltpu.VMEM((relations, nr - 1, prow, half), BF16),
            pltpu.VMEM((relations, prow, half), BF16),
            pltpu.VMEM((relations, nk, zrows, 128), BF16),
            dma(3), dma(SEMS), dma(SEMS),
        ],
        compiler_params=pltpu.CompilerParams(
            collective_id=0, has_side_effects=True, vmem_limit_bytes=67043328
        ),
    )(
        out_grad.T, node_in, tile_rows, tile_cols, tile_count.reshape(relations), tile_rows, tile_cols,
        weights, tile_vals.reshape(slots, tile, tile),
    )
    d_nodes, d_weights = widen(d_nodes, gathered)
    return d_nodes, d_weights.reshape(relations, f, f)


def solution(mesh):
    return jax.shard_map(
        functools.partial(body, mesh.shape["row"], mesh.shape["col"]),
        mesh=mesh,
        in_specs=(
            P("col", "row"),
            P(("row", "col"), None),
            P(),
            P(None, "col", "row", None, None, None),
            P(None, "col", "row", None),
            P(None, "col", "row", None),
            P(None, "col", "row"),
        ),
        out_specs=(P(("row", "col"), None), P()),
        check_vma=False,
    )
```

```python
import functools

import jax
import jax.numpy as jnp
from jax import lax
from jax.experimental import pallas as pl
from jax.experimental.pallas import tpu as pltpu
from jax.sharding import PartitionSpec as P

MESH = pl.DeviceIdType.MESH
F32 = jnp.float32
BF16 = jnp.bfloat16
SEMS = 360


def main_kernel(
    nr, nc, relations, cap,
    gin_ref, nodes_ref, rows_s, cols_s, count_s, rows_v, cols_v, w_hbm, t_hbm,
    dn_ref, ag_ref,
    gt, gy, w, tiles, tilest, xall, pm, acc, nsend, nrecv, nown, meta, link,
    zsa, zra, zsb, zrb, xs, xr, xf, dwrecv, pbuf, precv, zbuf, zrecv,
    load_sem, ssem, rsem,
):
    ny = nr // 2
    nz = nc // 4
    nk = nc // 2
    nd, f = nodes_ref.shape
    gb, tn = gin_ref.shape
    nt = tn // nd
    half = f // 2
    hb = half // nd
    me_r = lax.axis_index("row")
    me_c = lax.axis_index("col")
    xh = me_r // ny
    y = lax.rem(me_r, ny)
    xl = me_c // (2 * nz)
    z = lax.rem(me_c // 2, nz)
    core = lax.rem(me_c, 2)
    other = 1 - core

    def zat(dz):
        return lax.rem(z + (dz + 2 * nz), nz)

    def kat(x, zz):
        return x * nz + zz

    def cat(x, zz):
        return kat(x, zz) * 2 + core

    sibling = {"col": kat(xl, z) * 2 + other}
    xdev = {"col": cat(1 - xl, z)}
    xhdev = {"row": (1 - xh) * ny + y}

    def zdev(dz):
        return {"col": cat(xl, zat(dz))}

    def yat(dy):
        return lax.rem(y + (dy + 2 * ny), ny)

    def ydev(dy):
        return {"row": xh * ny + yat(dy)}

    def row_peer(d):
        r = lax.rem(me_r + d, nr)
        side = lax.rem(xl + xh + r // ny, 2)
        return {"row": r, "col": cat(side, z)}

    def k_peer(d):
        k = lax.rem(kat(xl, z) + d, nk)
        return k, {"col": k * 2 + core}

    used = [0]
    started = []

    def send(src, dst, dev):
        i = used[0]
        used[0] += 1
        c = pltpu.make_async_remote_copy(
            src_ref=src, dst_ref=dst, send_sem=ssem.at[i], recv_sem=rsem.at[i],
            device_id=dev, device_id_type=MESH,
        )
        c.start()
        started.append(c)
        return c

    load_w = pltpu.make_async_copy(w_hbm, w, load_sem.at[0])
    load_t = pltpu.make_async_copy(t_hbm, tiles, load_sem.at[1])
    load_t.start()
    load_w.start()

    barrier = pltpu.get_barrier_semaphore()
    for d in range(1, nr):
        pl.semaphore_signal(barrier, inc=1, device_id=row_peer(d), device_id_type=MESH)
    for d in range(1, nk):
        pl.semaphore_signal(barrier, inc=1, device_id=k_peer(d)[1], device_id_type=MESH)
    pl.semaphore_signal(barrier, inc=1, device_id=sibling, device_id_type=MESH)
    pl.semaphore_signal(barrier, inc=1, device_id=xhdev, device_id_type=MESH)
    pl.semaphore_wait(barrier, nr - 1 + nk - 1 + 2)

    def hops(n, orient, way):
        return n // 2 if way == orient else n - 1 - n // 2

    gh = gb // 2
    g_streams = {"o0": (0, 1), "o1": (1, -1), "p0": (0, 1), "p1": (1, -1)}

    def g_ref(st, dy):
        side = xh if st[0] == "o" else 1 - xh
        row = (side * ny + yat(dy)) * gb + g_streams[st][0] * gh
        return gt.at[pl.ds(pl.multiple_of(row, gh), gh), :]

    gcopy = {}

    def g_send(st, way, h):
        here = g_ref(st, -way * (h - 1))
        src = gin_ref.at[pl.ds(g_streams[st][0] * gh, gh), :] if h == 1 and st[0] == "o" else here
        gcopy[st, way, h] = send(src, here, ydev(way))

    def g_first(st):
        for way in (1, -1):
            if hops(ny, g_streams[st][1], way) >= 1:
                g_send(st, way, 1)

    def g_arrive(st, way, h):
        if (st, way, h) not in gcopy:
            return
        gcopy[st, way, h].wait_recv()
        if h < hops(ny, g_streams[st][1], way):
            g_send(st, way, h + 1)

    q = nd // 4
    x_streams = {"b0": (2 * q, q, 1), "b1": (3 * q, q, -1), "own": (0, 2 * q, 1), "par": (0, 2 * q, -1)}

    def x_rows(st):
        return slice(x_streams[st][0], x_streams[st][0] + x_streams[st][1])

    def x_ref(st, dz, x=None):
        if x is None:
            x = 1 - xl if st == "par" else xl
        return xall.at[cat(x, zat(dz)), x_rows(st), :]

    xcopy = {}
    xfwd = {}
    sib = []

    def to_sibling(ref):
        sib.append(send(ref, ref, sibling))

    def x_send(st, way, h):
        here = x_ref(st, -way * (h - 1))
        src = nodes_ref.at[x_rows(st), :] if h == 1 and st != "par" else here
        xcopy[st, way, h] = send(src, here, zdev(way))

    def x_first(st):
        for way in (1, -1):
            if hops(nz, x_streams[st][2], way) >= 1:
                x_send(st, way, 1)

    def x_arrive(st, way, h):
        if (st, way, h) not in xcopy:
            return
        xcopy[st, way, h].wait_recv()
        if h < hops(nz, x_streams[st][2], way):
            x_send(st, way, h + 1)
        here = x_ref(st, -way * h)
        if st[0] == "b":
            xfwd[st, way, h] = send(here, here, xdev)
        to_sibling(here)

    def x_cross(st, way, h):
        if (st, way, h) not in xfwd:
            return
        xfwd[st, way, h].wait_recv()
        to_sibling(x_ref(st, -way * h, 1 - xl))

    mine = xall.at[me_c]
    swap = send(nodes_ref.at[x_rows("par"), :], mine.at[x_rows("par"), :], xdev)
    for st in ("o0", "o1"):
        g_first(st)
    gswap = send(gin_ref, gt.at[pl.ds(pl.multiple_of(me_r * gb, gb), gb), :], xhdev)
    for st in ("b0", "b1", "own"):
        x_first(st)
    for st in ("b0", "b1"):
        xfwd[st, 0, 0] = send(nodes_ref.at[x_rows(st), :], mine.at[x_rows(st), :], xdev)
    sib.append(send(nodes_ref, mine, sibling))
    xall[me_c] = nodes_ref[...]
    gt[pl.ds(pl.multiple_of(me_r * gb, gb), gb), :] = gin_ref[...]

    slot_row = lax.broadcasted_iota(jnp.int32, (cap, cap), 0)
    slot_col = lax.broadcasted_iota(jnp.int32, (cap, cap), 1)
    places = lax.broadcasted_iota(jnp.int32, (cap, nc), 1)
    numbers = lax.broadcasted_iota(jnp.int32, (cap, nc), 0)

    def keys(ref, r):
        lane = lax.broadcasted_iota(jnp.int32, (1, cap), 1)
        key = jnp.where(lane < count_s[r], ref[r, 0], -1)
        turned = jnp.max(jnp.where(slot_row == slot_col, jnp.broadcast_to(key, (cap, cap)), -1), axis=1, keepdims=True)
        return key, turned

    def before(turned, key, offset, whole):
        same = turned == key
        if not whole:
            same = same & (slot_row < slot_col)
        return jnp.max(jnp.where(same, slot_row + (1 + offset), 0), axis=0, keepdims=True)

    def final(turned, offset):
        return jnp.max(jnp.where(turned == places, numbers + (1 + offset), 0), axis=0, keepdims=True)

    by_col = [keys(cols_v, r) for r in range(relations)]
    ends = final(by_col[0][1], 0)
    for r in range(1, relations):
        ends = jnp.maximum(ends, final(by_col[r][1], r * cap))
    meta[relations : relations + 1, 0:nc] = ends
    for r in range(relations):
        prior = before(by_col[r][1], by_col[r][0], r * cap, False)
        for e in range(r):
            prior = jnp.maximum(prior, before(by_col[e][1], by_col[r][0], e * cap, True))
        meta[r : r + 1, 0:cap] = prior
        key, turned = keys(rows_v, r)
        meta[4 + r : 5 + r, 0:cap] = before(turned, key, 0, False)
        meta[8 + r : 9 + r, 0:nc] = final(turned, 0)
    to_scalar = pltpu.make_async_copy(meta, link, load_sem.at[2])
    to_scalar.start()

    load_t.wait()

    def turn(r):
        def one(s, carry):
            tilest[r * cap + s] = tiles[r * cap + s].T
            return carry

        lax.fori_loop(0, cap, one, 0, unroll=16)

    turn(0)
    swap.wait_recv()
    to_sibling(x_ref("par", 0))
    x_first("par")
    gswap.wait_recv()
    for st in ("p0", "p1"):
        g_first(st)
    for way in (1, -1):
        for st in ("o0", "o1"):
            g_arrive(st, way, 1)
    turn(1)

    def x_round(h):
        for st in ("b0", "b1", "own", "par"):
            for way in (1, -1):
                x_arrive(st, way, h)
        for st in ("b0", "b1"):
            if h == 1:
                x_cross(st, 0, 0)
            for way in (1, -1):
                x_cross(st, way, h - 1)

    x_round(1)
    turn(2)
    for way in (1, -1):
        for st in ("p0", "p1"):
            g_arrive(st, way, 1)
    x_round(2)
    for h in range(2, ny):
        for way in (1, -1):
            for st in g_streams:
                g_arrive(st, way, h)
    load_w.wait()
    x_round(3)
    to_scalar.wait()

    for b in range(f // nd):
        gy[:, b * nd : (b + 1) * nd] = gt[b * nd : (b + 1) * nd, :].T
    for r in range(relations):
        prod = lax.dot_general(
            gy[...], w[r], (((1,), (1,)), ((), ())), preferred_element_type=F32
        ).astype(BF16)
        for i in range(nt):
            pm[r * nt + i] = prod[i * nd : (i + 1) * nd, :]
    acc[0] = jnp.zeros((nd, f), F32)

    def mix(r):
        def one(s, carry):
            t = r * cap + s
            p = jnp.dot(tilest[t], pm[r * nt + rows_s[r, 0, 0, s]], preferred_element_type=F32)
            acc[t + 1] = p + acc[link[r, s]]
            return carry

        lax.fori_loop(0, cap, one, 0, unroll=16)

    mix(0)
    mix(1)
    x_round(4)
    mix(2)

    order = [nz // 2]
    for d in range(nz // 2 - 1, 0, -1):
        order += [d, -d]
    order.append(0)
    ncore = {}
    for dz in order:
        for x in (0, 1):
            k = kat(1 - xl if x == 0 else xl, zat(dz))
            nsend[k] = acc[link[relations, 2 * k + other]]
            ncore[dz, x] = send(nsend.at[k], nrecv.at[k], sibling)

    xcross = {}

    def n_core(dz):
        for x in (0, 1):
            ncore[dz, x].wait_recv()
            k = kat(1 - xl if x == 0 else xl, zat(dz))
            nown[k] = nown[k] + nrecv[k]
        slot = zat(dz)
        xs[slot] = nown[kat(1 - xl, slot), 2 * q :, :].astype(BF16)
        xcross[dz] = send(xs.at[slot], xr.at[slot], xdev)

    def n_cross(dz):
        xcross[dz].wait_recv()
        k = kat(xl, zat(dz))
        nown[k, 2 * q :, :] = nown[k, 2 * q :, :] + xr[zat(dz)].astype(F32)

    zcopy = {}
    parts = {"par": (zsa, zra, 0), "own": (zsa, zra, 1), "b0": (zsb, zrb, 0), "b1": (zsb, zrb, 1)}

    def n_send(st, way, t):
        n = hops(nz, x_streams[st][2], way)
        if t > n:
            return
        sbuf, rbuf, slot = parts[st]
        side = 0 if way == 1 else 1
        x = 1 - xl if st == "par" else xl
        value = nown[kat(x, zat(way * (n + 1 - t))), x_rows(st), :]
        if t > 1:
            zcopy[st, way, t - 1].wait_recv()
            value = value + rbuf[slot, side, t - 2].astype(F32)
        sbuf[slot, side, t - 1] = value.astype(BF16)
        zcopy[st, way, t] = send(sbuf.at[slot, side, t - 1], rbuf.at[slot, side, t - 1], zdev(way))

    def n_final(st):
        x = 1 - xl if st == "par" else xl
        value = nown[kat(x, z), x_rows(st), :]
        for way in (1, -1):
            n = hops(nz, x_streams[st][2], way)
            if n:
                zcopy[st, way, n].wait_recv()
                _, rbuf, slot = parts[st]
                value = value + rbuf[slot, 0 if way == 1 else 1, n - 1].astype(F32)
        return value

    def n_round(t, names):
        for st in names:
            for way in (1, -1):
                n_send(st, way, t)

    base = cap + 1
    blocks = f // nd

    def terms(r):
        def one(s, carry):
            t = r * cap + s
            p = jnp.dot(tiles[t], xall[cols_s[r, 0, 0, s]], preferred_element_type=F32)
            acc[s + 1] = p + acc[link[4 + r, s]]
            return carry

        lax.fori_loop(0, cap, one, 0, unroll=16)
        for i in range(nt):
            gy[i * nd : (i + 1) * nd, :] = acc[link[8 + r, i]].astype(BF16)

    batches = {}

    def product(r):
        for b in range(blocks):
            acc[base + r * blocks + b] = jnp.dot(
                gt[b * nd : (b + 1) * nd, :], gy[...], preferred_element_type=F32
            )
        src = acc.at[pl.ds(base + r * blocks + other * hb, hb)]
        batches[0, r] = [send(src, dwrecv.at[r], sibling)]

    def arrived(stage, r):
        for c in batches[stage, r]:
            c.wait_recv()

    prow = f // nr

    def plane_scatter(r):
        arrived(0, r)
        for b in range(hb):
            total = acc[base + r * blocks + core * hb + b] + dwrecv[r, b]
            pbuf[r, :, b * nd : (b + 1) * nd] = total.astype(BF16).T
        copies = []
        for d in range(1, nr):
            peer = lax.rem(me_r + d, nr)
            src = pbuf.at[r, pl.ds(pl.multiple_of(peer * prow, prow), prow), :]
            copies.append(send(src, precv.at[r, d - 1], row_peer(d)))
        batches[1, r] = copies

    lanes = half // 128
    zrows = prow * lanes // nz

    def piece(zz):
        row = pl.multiple_of((zz // lanes) * zrows, zrows)
        lane = pl.multiple_of(lax.rem(zz, lanes) * 128, 128)
        return row, lane

    def z_scatter(r):
        arrived(1, r)
        part = pbuf[r, pl.ds(pl.multiple_of(me_r * prow, prow), prow), :].astype(F32)
        for d in range(1, nr):
            part = part + precv[r, d - 1].astype(F32)
        zbuf[r] = part.astype(BF16)
        me_k = kat(xl, z)
        row, lane = piece(z)
        zrecv[r, me_k] = zbuf[r, pl.ds(row, zrows), pl.ds(lane, 128)]
        copies = []
        for d in range(1, nk):
            k, dev = k_peer(d)
            row, lane = piece(lax.rem(k, nz))
            src = zbuf.at[r, pl.ds(row, zrows), pl.ds(lane, 128)]
            copies.append(send(src, zrecv.at[r, me_k], dev))
        batches[2, r] = copies

    def z_gather(r):
        arrived(2, r)
        final = zrecv[r, 0].astype(F32)
        for k in range(1, nk):
            final = final + zrecv[r, k].astype(F32)
        row, lane = piece(z)
        row = pl.multiple_of(r * f + me_r * prow + row, zrows)
        lane = pl.multiple_of(core * half + lane, 128)
        ag_ref[pl.ds(row, zrows), pl.ds(lane, 128)] = final.astype(BF16)
        mine = ag_ref.at[pl.ds(row, zrows), pl.ds(lane, 128)]
        batches[3, r] = [send(mine, mine, zdev(d)) for d in range(1, nz)]

    def strip(r, who):
        row = pl.multiple_of(r * f + who * prow, prow)
        return ag_ref.at[pl.ds(row, prow), pl.ds(pl.multiple_of(core * half, half), half)]

    last = []

    def plane_gather(r):
        arrived(3, r)
        mine = strip(r, me_r)
        batches[4, r] = [send(mine, mine, row_peer(d)) for d in range(1, nr)]
        last.append(send(mine, mine, sibling))

    def core_gather(r):
        for d in range(1, nr):
            batches[4, r][d - 1].wait_recv()
            there = strip(r, lax.rem(me_r + nr - d, nr))
            last.append(send(there, there, sibling))

    first = [d for d in order if abs(d) >= nz // 2 - 1]
    rest = [d for d in order if d not in first]
    a_names, b_names = ("par", "own"), ("b0", "b1")

    def keep(k, carry):
        nown[k] = acc[link[relations, 2 * k + core]]
        return carry

    lax.fori_loop(0, nk, keep, 0)
    for dz in first:
        n_core(dz)
    n_round(1, a_names)
    for h in range(5, nz + 1):
        x_round(h)
    for dz in rest:
        n_core(dz)
    for c in sib:
        c.wait_recv()
    near = [d for d in rest if abs(d) == nz // 2 - 2]
    nearer = [d for d in rest if d not in near and d != 0]
    last_cross = [d for d in rest if d not in near and d not in nearer]
    terms(0)
    product(0)
    for dz in first:
        n_cross(dz)
    n_round(1, b_names)
    terms(1)
    product(1)
    plane_scatter(0)
    n_round(2, a_names)
    terms(2)
    product(2)
    plane_scatter(1)
    plane_scatter(2)
    for dz in near:
        n_cross(dz)
    n_round(2, b_names)
    n_round(3, a_names)
    for r in range(relations):
        z_scatter(r)
    for r in range(relations):
        z_gather(r)
    for dz in nearer:
        n_cross(dz)
    n_round(3, b_names)
    for t in range(4, nz):
        n_round(t, a_names)
    for r in range(relations):
        plane_gather(r)
    xf[0] = n_final("par").astype(BF16)
    xlast = send(xf.at[0], xf.at[1], xdev)
    for dz in last_cross:
        n_cross(dz)
    for t in range(4, nz):
        n_round(t, b_names)
    core_gather(0)
    core_gather(1)
    for st in b_names:
        dn_ref[x_rows(st), :] = n_final(st).astype(BF16)
    own = n_final("own")
    xlast.wait_recv()
    dn_ref[x_rows("own"), :] = (own + xf[1].astype(F32)).astype(BF16)
    core_gather(2)
    for c in last:
        c.wait_recv()
    for c in started:
        c.wait_send()
    assert used[0] <= SEMS


def widen_kernel(dn_ref, dw_ref, dn_out, dw_out, nodes, narrow, wide, in_sem, out_sem):
    parts, rows = narrow.shape[0], narrow.shape[1]

    def part(ref, k):
        return ref.at[k * rows : (k + 1) * rows, :]

    loads = [pltpu.make_async_copy(part(dw_ref, k), narrow.at[k], in_sem.at[k]) for k in range(parts)]
    stores = [pltpu.make_async_copy(wide.at[k], part(dw_out, k), out_sem.at[k]) for k in range(parts)]
    loads.append(pltpu.make_async_copy(dn_ref, nodes, in_sem.at[parts]))
    stores.append(pltpu.make_async_copy(nodes, dn_out, out_sem.at[parts]))
    for c in loads:
        c.start()
    for k in range(parts):
        loads[k].wait()
        wide[k] = narrow[k].astype(F32)
        stores[k].start()
    loads[parts].wait()
    stores[parts].start()
    for c in stores:
        c.wait()


def widen(d_nodes, gathered):
    total, f = gathered.shape
    parts = 6 if total % 96 == 0 else 1
    rows = total // parts
    hbm = pl.BlockSpec(memory_space=pltpu.HBM)
    return pl.pallas_call(
        widen_kernel,
        in_specs=[hbm, hbm],
        out_specs=(hbm, hbm),
        out_shape=(
            jax.ShapeDtypeStruct(d_nodes.shape, BF16),
            jax.ShapeDtypeStruct(gathered.shape, F32),
        ),
        scratch_shapes=[
            pltpu.VMEM(d_nodes.shape, BF16),
            pltpu.VMEM((parts, rows, f), BF16),
            pltpu.VMEM((parts, rows, f), F32),
            pltpu.SemaphoreType.DMA((parts + 1,)),
            pltpu.SemaphoreType.DMA((parts + 1,)),
        ],
    )(d_nodes, gathered)


def body(nr, nc, out_grad, node_in, weights, tile_vals, tile_rows, tile_cols, tile_count):
    relations, f = weights.shape[0], weights.shape[1]
    tn, width = out_grad.shape
    nd = node_in.shape[0]
    cap, tile = tile_vals.shape[3], tile_vals.shape[4]
    slots = relations * cap
    nt, nz, nk = tn // nd, nc // 4, nc // 2
    half = f // 2
    hb = half // nd
    prow = f // nr
    q = nd // 4
    hop = max(nz // 2, 1)
    zrows = prow * (half // 128) // nz

    dma = lambda *n: pltpu.SemaphoreType.DMA(n)
    vmem = pl.BlockSpec(memory_space=pltpu.VMEM)
    smem = pl.BlockSpec(memory_space=pltpu.SMEM)
    hbm = pl.BlockSpec(memory_space=pltpu.HBM)
    d_nodes, gathered = pl.pallas_call(
        functools.partial(main_kernel, nr, nc, relations, cap),
        out_shape=(
            jax.ShapeDtypeStruct((nd, f), BF16),
            jax.ShapeDtypeStruct((relations * f, f), BF16),
        ),
        in_specs=[vmem, vmem, smem, smem, smem, vmem, vmem, hbm, hbm],
        out_specs=(vmem, vmem),
        scratch_shapes=[
            pltpu.VMEM((f, tn), BF16),
            pltpu.VMEM((tn, f), BF16),
            pltpu.VMEM(weights.shape, BF16),
            pltpu.VMEM((slots, tile, tile), BF16),
            pltpu.VMEM((slots, tile, tile), BF16),
            pltpu.VMEM((nc, nd, f), BF16),
            pltpu.VMEM((relations * nt, nd, f), BF16),
            pltpu.VMEM((slots + 1, nd, f), F32),
            pltpu.VMEM((nk, nd, f), F32),
            pltpu.VMEM((nk, nd, f), F32),
            pltpu.VMEM((nk, nd, f), F32),
            pltpu.VMEM((16, 128), jnp.int32),
            pltpu.SMEM((16, 128), jnp.int32),
            pltpu.VMEM((2, 2, hop, 2 * q, f), BF16),
            pltpu.VMEM((2, 2, hop, 2 * q, f), BF16),
            pltpu.VMEM((2, 2, hop, q, f), BF16),
            pltpu.VMEM((2, 2, hop, q, f), BF16),
            pltpu.VMEM((nz, 2 * q, f), BF16),
            pltpu.VMEM((nz, 2 * q, f), BF16),
            pltpu.VMEM((2, 2 * q, f), BF16),
            pltpu.VMEM((relations, hb, nd, f), F32),
            pltpu.VMEM((relations, f, half), BF16),
            pltpu.VMEM((relations, nr - 1, prow, half), BF16),
            pltpu.VMEM((relations, prow, half), BF16),
            pltpu.VMEM((relations, nk, zrows, 128), BF16),
            dma(3), dma(SEMS), dma(SEMS),
        ],
        compiler_params=pltpu.CompilerParams(
            collective_id=0, has_side_effects=True, vmem_limit_bytes=67043328
        ),
    )(
        out_grad.T, node_in, tile_rows, tile_cols, tile_count.reshape(relations), tile_rows, tile_cols,
        weights, tile_vals.reshape(slots, tile, tile),
    )
    d_nodes, d_weights = widen(d_nodes, gathered)
    return d_nodes, d_weights.reshape(relations, f, f)


def solution(mesh):
    return jax.shard_map(
        functools.partial(body, mesh.shape["row"], mesh.shape["col"]),
        mesh=mesh,
        in_specs=(
            P("col", "row"),
            P(("row", "col"), None),
            P(),
            P(None, "col", "row", None, None, None),
            P(None, "col", "row", None),
            P(None, "col", "row", None),
            P(None, "col", "row"),
        ),
        out_specs=(P(("row", "col"), None), P()),
        check_vma=False,
    )
```

```python
import functools

import jax
import jax.numpy as jnp
from jax import lax
from jax.experimental import pallas as pl
from jax.experimental.pallas import tpu as pltpu
from jax.sharding import PartitionSpec as P

MESH = pl.DeviceIdType.MESH
F32 = jnp.float32
BF16 = jnp.bfloat16
SEMS = 360


def main_kernel(
    nr, nc, relations, cap,
    gin_ref, nodes_ref, rows_s, cols_s, count_s, rows_v, cols_v, w_hbm, t_hbm,
    dn_out, ag_out,
    dn_ref, ag_ref, gt, gy, w, tiles, tilest, xall, pm, acc, nsend, nrecv, nown, meta, link,
    zsa, zra, zsb, zrb, xs, xr, xf, dwrecv, pbuf, precv, zbuf, zrecv,
    load_sem, ssem, rsem,
):
    ny = nr // 2
    nz = nc // 4
    nk = nc // 2
    nd, f = nodes_ref.shape
    gb, tn = gin_ref.shape
    nt = tn // nd
    half = f // 2
    hb = half // nd
    me_r = lax.axis_index("row")
    me_c = lax.axis_index("col")
    xh = me_r // ny
    y = lax.rem(me_r, ny)
    xl = me_c // (2 * nz)
    z = lax.rem(me_c // 2, nz)
    core = lax.rem(me_c, 2)
    other = 1 - core

    def zat(dz):
        return lax.rem(z + (dz + 2 * nz), nz)

    def kat(x, zz):
        return x * nz + zz

    def cat(x, zz):
        return kat(x, zz) * 2 + core

    sibling = {"col": kat(xl, z) * 2 + other}
    xdev = {"col": cat(1 - xl, z)}
    xhdev = {"row": (1 - xh) * ny + y}

    def zdev(dz):
        return {"col": cat(xl, zat(dz))}

    def yat(dy):
        return lax.rem(y + (dy + 2 * ny), ny)

    def ydev(dy):
        return {"row": xh * ny + yat(dy)}

    def row_peer(d):
        r = lax.rem(me_r + d, nr)
        side = lax.rem(xl + xh + r // ny, 2)
        return {"row": r, "col": cat(side, z)}

    def k_peer(d):
        k = lax.rem(kat(xl, z) + d, nk)
        return k, {"col": k * 2 + core}

    used = [0]
    started = []

    def send(src, dst, dev):
        i = used[0]
        used[0] += 1
        c = pltpu.make_async_remote_copy(
            src_ref=src, dst_ref=dst, send_sem=ssem.at[i], recv_sem=rsem.at[i],
            device_id=dev, device_id_type=MESH,
        )
        c.start()
        started.append(c)
        return c

    load_w = pltpu.make_async_copy(w_hbm, w, load_sem.at[0])
    load_t = pltpu.make_async_copy(t_hbm, tiles, load_sem.at[1])
    load_t.start()
    load_w.start()

    barrier = pltpu.get_barrier_semaphore()
    for d in range(1, nr):
        pl.semaphore_signal(barrier, inc=1, device_id=row_peer(d), device_id_type=MESH)
    for d in range(1, nk):
        pl.semaphore_signal(barrier, inc=1, device_id=k_peer(d)[1], device_id_type=MESH)
    pl.semaphore_signal(barrier, inc=1, device_id=sibling, device_id_type=MESH)
    pl.semaphore_signal(barrier, inc=1, device_id=xhdev, device_id_type=MESH)
    pl.semaphore_wait(barrier, nr - 1 + nk - 1 + 2)

    def hops(n, orient, way):
        return n // 2 if way == orient else n - 1 - n // 2

    gh = gb // 2
    g_streams = {"o0": (0, 1), "o1": (1, -1), "p0": (0, 1), "p1": (1, -1)}

    def g_ref(st, dy):
        side = xh if st[0] == "o" else 1 - xh
        row = (side * ny + yat(dy)) * gb + g_streams[st][0] * gh
        return gt.at[pl.ds(pl.multiple_of(row, gh), gh), :]

    gcopy = {}

    def g_send(st, way, h):
        here = g_ref(st, -way * (h - 1))
        src = gin_ref.at[pl.ds(g_streams[st][0] * gh, gh), :] if h == 1 and st[0] == "o" else here
        gcopy[st, way, h] = send(src, here, ydev(way))

    def g_first(st):
        for way in (1, -1):
            if hops(ny, g_streams[st][1], way) >= 1:
                g_send(st, way, 1)

    def g_arrive(st, way, h):
        if (st, way, h) not in gcopy:
            return
        gcopy[st, way, h].wait_recv()
        if h < hops(ny, g_streams[st][1], way):
            g_send(st, way, h + 1)

    q = nd // 4
    x_streams = {"b0": (2 * q, q, 1), "b1": (3 * q, q, -1), "own": (0, 2 * q, 1), "par": (0, 2 * q, -1)}

    def x_rows(st):
        return slice(x_streams[st][0], x_streams[st][0] + x_streams[st][1])

    def x_ref(st, dz, x=None):
        if x is None:
            x = 1 - xl if st == "par" else xl
        return xall.at[cat(x, zat(dz)), x_rows(st), :]

    xcopy = {}
    xfwd = {}
    sib = []

    def to_sibling(ref):
        sib.append(send(ref, ref, sibling))

    def x_send(st, way, h):
        here = x_ref(st, -way * (h - 1))
        src = nodes_ref.at[x_rows(st), :] if h == 1 and st != "par" else here
        xcopy[st, way, h] = send(src, here, zdev(way))

    def x_first(st):
        for way in (1, -1):
            if hops(nz, x_streams[st][2], way) >= 1:
                x_send(st, way, 1)

    def x_arrive(st, way, h):
        if (st, way, h) not in xcopy:
            return
        xcopy[st, way, h].wait_recv()
        if h < hops(nz, x_streams[st][2], way):
            x_send(st, way, h + 1)
        here = x_ref(st, -way * h)
        if st[0] == "b":
            xfwd[st, way, h] = send(here, here, xdev)
        to_sibling(here)

    def x_cross(st, way, h):
        if (st, way, h) not in xfwd:
            return
        xfwd[st, way, h].wait_recv()
        to_sibling(x_ref(st, -way * h, 1 - xl))

    mine = xall.at[me_c]
    swap = send(nodes_ref.at[x_rows("par"), :], mine.at[x_rows("par"), :], xdev)
    for st in ("o0", "o1"):
        g_first(st)
    gswap = send(gin_ref, gt.at[pl.ds(pl.multiple_of(me_r * gb, gb), gb), :], xhdev)
    for st in ("b0", "b1", "own"):
        x_first(st)
    for st in ("b0", "b1"):
        xfwd[st, 0, 0] = send(nodes_ref.at[x_rows(st), :], mine.at[x_rows(st), :], xdev)
    sib.append(send(nodes_ref, mine, sibling))
    xall[me_c] = nodes_ref[...]
    gt[pl.ds(pl.multiple_of(me_r * gb, gb), gb), :] = gin_ref[...]

    slot_row = lax.broadcasted_iota(jnp.int32, (cap, cap), 0)
    slot_col = lax.broadcasted_iota(jnp.int32, (cap, cap), 1)
    places = lax.broadcasted_iota(jnp.int32, (cap, nc), 1)
    numbers = lax.broadcasted_iota(jnp.int32, (cap, nc), 0)

    def keys(ref, r):
        lane = lax.broadcasted_iota(jnp.int32, (1, cap), 1)
        key = jnp.where(lane < count_s[r], ref[r, 0], -1)
        turned = jnp.max(jnp.where(slot_row == slot_col, jnp.broadcast_to(key, (cap, cap)), -1), axis=1, keepdims=True)
        return key, turned

    def before(turned, key, offset, whole):
        same = turned == key
        if not whole:
            same = same & (slot_row < slot_col)
        return jnp.max(jnp.where(same, slot_row + (1 + offset), 0), axis=0, keepdims=True)

    def final(turned, offset):
        return jnp.max(jnp.where(turned == places, numbers + (1 + offset), 0), axis=0, keepdims=True)

    by_col = [keys(cols_v, r) for r in range(relations)]
    ends = final(by_col[0][1], 0)
    for r in range(1, relations):
        ends = jnp.maximum(ends, final(by_col[r][1], r * cap))
    meta[relations : relations + 1, 0:nc] = ends
    for r in range(relations):
        prior = before(by_col[r][1], by_col[r][0], r * cap, False)
        for e in range(r):
            prior = jnp.maximum(prior, before(by_col[e][1], by_col[r][0], e * cap, True))
        meta[r : r + 1, 0:cap] = prior
        key, turned = keys(rows_v, r)
        meta[4 + r : 5 + r, 0:cap] = before(turned, key, 0, False)
        meta[8 + r : 9 + r, 0:nc] = final(turned, 0)
    to_scalar = pltpu.make_async_copy(meta, link, load_sem.at[2])
    to_scalar.start()

    load_t.wait()

    def turn(r):
        def one(s, carry):
            tilest[r * cap + s] = tiles[r * cap + s].T
            return carry

        lax.fori_loop(0, cap, one, 0, unroll=16)

    turn(0)
    swap.wait_recv()
    to_sibling(x_ref("par", 0))
    x_first("par")
    gswap.wait_recv()
    for st in ("p0", "p1"):
        g_first(st)
    for way in (1, -1):
        for st in ("o0", "o1"):
            g_arrive(st, way, 1)
    turn(1)

    def x_round(h):
        for st in ("b0", "b1", "own", "par"):
            for way in (1, -1):
                x_arrive(st, way, h)
        for st in ("b0", "b1"):
            if h == 1:
                x_cross(st, 0, 0)
            for way in (1, -1):
                x_cross(st, way, h - 1)

    x_round(1)
    turn(2)
    for way in (1, -1):
        for st in ("p0", "p1"):
            g_arrive(st, way, 1)
    x_round(2)
    for h in range(2, ny):
        for way in (1, -1):
            for st in g_streams:
                g_arrive(st, way, h)
    load_w.wait()
    x_round(3)
    to_scalar.wait()

    for b in range(f // nd):
        gy[:, b * nd : (b + 1) * nd] = gt[b * nd : (b + 1) * nd, :].T
    for r in range(relations):
        prod = lax.dot_general(
            gy[...], w[r], (((1,), (1,)), ((), ())), preferred_element_type=F32
        ).astype(BF16)
        for i in range(nt):
            pm[r * nt + i] = prod[i * nd : (i + 1) * nd, :]
    acc[0] = jnp.zeros((nd, f), F32)

    def mix(r):
        def one(s, carry):
            t = r * cap + s
            p = jnp.dot(tilest[t], pm[r * nt + rows_s[r, 0, 0, s]], preferred_element_type=F32)
            acc[t + 1] = p + acc[link[r, s]]
            return carry

        lax.fori_loop(0, cap, one, 0, unroll=16)

    mix(0)
    mix(1)
    x_round(4)
    mix(2)

    order = [nz // 2]
    for d in range(nz // 2 - 1, 0, -1):
        order += [d, -d]
    order.append(0)
    ncore = {}
    for dz in order:
        for x in (0, 1):
            k = kat(1 - xl if x == 0 else xl, zat(dz))
            nsend[k] = acc[link[relations, 2 * k + other]]
            ncore[dz, x] = send(nsend.at[k], nrecv.at[k], sibling)

    xcross = {}

    def n_core(dz):
        for x in (0, 1):
            ncore[dz, x].wait_recv()
            k = kat(1 - xl if x == 0 else xl, zat(dz))
            nown[k] = nown[k] + nrecv[k]
        slot = zat(dz)
        xs[slot] = nown[kat(1 - xl, slot), 2 * q :, :].astype(BF16)
        xcross[dz] = send(xs.at[slot], xr.at[slot], xdev)

    def n_cross(dz):
        xcross[dz].wait_recv()
        k = kat(xl, zat(dz))
        nown[k, 2 * q :, :] = nown[k, 2 * q :, :] + xr[zat(dz)].astype(F32)

    zcopy = {}
    parts = {"par": (zsa, zra, 0), "own": (zsa, zra, 1), "b0": (zsb, zrb, 0), "b1": (zsb, zrb, 1)}

    def n_send(st, way, t):
        n = hops(nz, x_streams[st][2], way)
        if t > n:
            return
        sbuf, rbuf, slot = parts[st]
        side = 0 if way == 1 else 1
        x = 1 - xl if st == "par" else xl
        value = nown[kat(x, zat(way * (n + 1 - t))), x_rows(st), :]
        if t > 1:
            zcopy[st, way, t - 1].wait_recv()
            value = value + rbuf[slot, side, t - 2].astype(F32)
        sbuf[slot, side, t - 1] = value.astype(BF16)
        zcopy[st, way, t] = send(sbuf.at[slot, side, t - 1], rbuf.at[slot, side, t - 1], zdev(way))

    def n_final(st):
        x = 1 - xl if st == "par" else xl
        value = nown[kat(x, z), x_rows(st), :]
        for way in (1, -1):
            n = hops(nz, x_streams[st][2], way)
            if n:
                zcopy[st, way, n].wait_recv()
                _, rbuf, slot = parts[st]
                value = value + rbuf[slot, 0 if way == 1 else 1, n - 1].astype(F32)
        return value

    def n_round(t, names):
        for st in names:
            for way in (1, -1):
                n_send(st, way, t)

    base = cap + 1
    blocks = f // nd

    def terms(r):
        def one(s, carry):
            t = r * cap + s
            p = jnp.dot(tiles[t], xall[cols_s[r, 0, 0, s]], preferred_element_type=F32)
            acc[s + 1] = p + acc[link[4 + r, s]]
            return carry

        lax.fori_loop(0, cap, one, 0, unroll=16)
        for i in range(nt):
            gy[i * nd : (i + 1) * nd, :] = acc[link[8 + r, i]].astype(BF16)

    batches = {}

    def product(r):
        for b in range(blocks):
            acc[base + r * blocks + b] = jnp.dot(
                gt[b * nd : (b + 1) * nd, :], gy[...], preferred_element_type=F32
            )
        src = acc.at[pl.ds(base + r * blocks + other * hb, hb)]
        batches[0, r] = [send(src, dwrecv.at[r], sibling)]

    def arrived(stage, r):
        for c in batches[stage, r]:
            c.wait_recv()

    prow = f // nr

    def plane_scatter(r):
        arrived(0, r)
        for b in range(hb):
            total = acc[base + r * blocks + core * hb + b] + dwrecv[r, b]
            pbuf[r, :, b * nd : (b + 1) * nd] = total.astype(BF16).T
        copies = []
        for d in range(1, nr):
            peer = lax.rem(me_r + d, nr)
            src = pbuf.at[r, pl.ds(pl.multiple_of(peer * prow, prow), prow), :]
            copies.append(send(src, precv.at[r, d - 1], row_peer(d)))
        batches[1, r] = copies

    lanes = half // 128
    zrows = prow * lanes // nz

    def piece(zz):
        row = pl.multiple_of((zz // lanes) * zrows, zrows)
        lane = pl.multiple_of(lax.rem(zz, lanes) * 128, 128)
        return row, lane

    def z_scatter(r):
        arrived(1, r)
        part = pbuf[r, pl.ds(pl.multiple_of(me_r * prow, prow), prow), :].astype(F32)
        for d in range(1, nr):
            part = part + precv[r, d - 1].astype(F32)
        zbuf[r] = part.astype(BF16)
        me_k = kat(xl, z)
        row, lane = piece(z)
        zrecv[r, me_k] = zbuf[r, pl.ds(row, zrows), pl.ds(lane, 128)]
        copies = []
        for d in range(1, nk):
            k, dev = k_peer(d)
            row, lane = piece(lax.rem(k, nz))
            src = zbuf.at[r, pl.ds(row, zrows), pl.ds(lane, 128)]
            copies.append(send(src, zrecv.at[r, me_k], dev))
        batches[2, r] = copies

    def z_gather(r):
        arrived(2, r)
        final = zrecv[r, 0].astype(F32)
        for k in range(1, nk):
            final = final + zrecv[r, k].astype(F32)
        row, lane = piece(z)
        row = pl.multiple_of(r * f + me_r * prow + row, zrows)
        lane = pl.multiple_of(core * half + lane, 128)
        ag_ref[pl.ds(row, zrows), pl.ds(lane, 128)] = final.astype(BF16)
        mine = ag_ref.at[pl.ds(row, zrows), pl.ds(lane, 128)]
        batches[3, r] = [send(mine, mine, zdev(d)) for d in range(1, nz)]

    def strip(r, who):
        row = pl.multiple_of(r * f + who * prow, prow)
        return ag_ref.at[pl.ds(row, prow), pl.ds(pl.multiple_of(core * half, half), half)]

    last = [[] for _ in range(relations)]

    def plane_gather(r):
        arrived(3, r)
        mine = strip(r, me_r)
        batches[4, r] = [send(mine, mine, row_peer(d)) for d in range(1, nr)]
        last[r].append(send(mine, mine, sibling))

    def core_gather(r):
        for d in range(1, nr):
            batches[4, r][d - 1].wait_recv()
            there = strip(r, lax.rem(me_r + nr - d, nr))
            last[r].append(send(there, there, sibling))

    first = [d for d in order if abs(d) >= nz // 2 - 1]
    rest = [d for d in order if d not in first]
    a_names, b_names = ("par", "own"), ("b0", "b1")

    def keep(k, carry):
        nown[k] = acc[link[relations, 2 * k + core]]
        return carry

    lax.fori_loop(0, nk, keep, 0)
    for dz in first:
        n_core(dz)
    n_round(1, a_names)
    for h in range(5, nz + 1):
        x_round(h)
    for dz in rest:
        n_core(dz)
    for c in sib:
        c.wait_recv()
    near = [d for d in rest if abs(d) == nz // 2 - 2]
    nearer = [d for d in rest if d not in near and d != 0]
    last_cross = [d for d in rest if d not in near and d not in nearer]
    terms(0)
    product(0)
    for dz in first:
        n_cross(dz)
    n_round(1, b_names)
    terms(1)
    product(1)
    plane_scatter(0)
    n_round(2, a_names)
    terms(2)
    product(2)
    plane_scatter(1)
    plane_scatter(2)
    for dz in near:
        n_cross(dz)
    n_round(2, b_names)
    n_round(3, a_names)
    for r in range(relations):
        z_scatter(r)
    for r in range(relations):
        z_gather(r)
    for dz in nearer:
        n_cross(dz)
    n_round(3, b_names)
    for t in range(4, nz):
        n_round(t, a_names)
    for r in range(relations):
        plane_gather(r)
    xf[0] = n_final("par").astype(BF16)
    xlast = send(xf.at[0], xf.at[1], xdev)
    for dz in last_cross:
        n_cross(dz)
    for t in range(4, nz):
        n_round(t, b_names)
    core_gather(0)
    core_gather(1)
    for st in b_names:
        dn_ref[x_rows(st), :] = n_final(st).astype(BF16)
    own = n_final("own")
    xlast.wait_recv()
    dn_ref[x_rows("own"), :] = (own + xf[1].astype(F32)).astype(BF16)
    core_gather(2)
    out = [pltpu.make_async_copy(dn_ref, dn_out, load_sem.at[3])]
    out[0].start()
    for r in range(relations):
        for c in last[r]:
            c.wait_recv()
        block = pl.ds(r * f, f)
        out.append(pltpu.make_async_copy(ag_ref.at[block, :], ag_out.at[block, :], load_sem.at[4 + r]))
        out[-1].start()
    for c in out:
        c.wait()
    for c in started:
        c.wait_send()
    assert used[0] <= SEMS


def widen_kernel(dn_ref, dw_ref, dn_out, dw_out, nodes, narrow, wide, in_sem, out_sem):
    parts, rows = narrow.shape[0], narrow.shape[1]

    def part(ref, k):
        return ref.at[k * rows : (k + 1) * rows, :]

    loads = [pltpu.make_async_copy(part(dw_ref, k), narrow.at[k], in_sem.at[k]) for k in range(parts)]
    stores = [pltpu.make_async_copy(wide.at[k], part(dw_out, k), out_sem.at[k]) for k in range(parts)]
    loads.append(pltpu.make_async_copy(dn_ref, nodes, in_sem.at[parts]))
    stores.append(pltpu.make_async_copy(nodes, dn_out, out_sem.at[parts]))
    for c in loads:
        c.start()
    for k in range(parts):
        loads[k].wait()
        wide[k] = narrow[k].astype(F32)
        stores[k].start()
    loads[parts].wait()
    stores[parts].start()
    for c in stores:
        c.wait()


def widen(d_nodes, gathered):
    total, f = gathered.shape
    parts = 6 if total % 96 == 0 else 1
    rows = total // parts
    hbm = pl.BlockSpec(memory_space=pltpu.HBM)
    return pl.pallas_call(
        widen_kernel,
        in_specs=[hbm, hbm],
        out_specs=(hbm, hbm),
        out_shape=(
            jax.ShapeDtypeStruct(d_nodes.shape, BF16),
            jax.ShapeDtypeStruct(gathered.shape, F32),
        ),
        scratch_shapes=[
            pltpu.VMEM(d_nodes.shape, BF16),
            pltpu.VMEM((parts, rows, f), BF16),
            pltpu.VMEM((parts, rows, f), F32),
            pltpu.SemaphoreType.DMA((parts + 1,)),
            pltpu.SemaphoreType.DMA((parts + 1,)),
        ],
    )(d_nodes, gathered)


def body(nr, nc, out_grad, node_in, weights, tile_vals, tile_rows, tile_cols, tile_count):
    relations, f = weights.shape[0], weights.shape[1]
    tn, width = out_grad.shape
    nd = node_in.shape[0]
    cap, tile = tile_vals.shape[3], tile_vals.shape[4]
    slots = relations * cap
    nt, nz, nk = tn // nd, nc // 4, nc // 2
    half = f // 2
    hb = half // nd
    prow = f // nr
    q = nd // 4
    hop = max(nz // 2, 1)
    zrows = prow * (half // 128) // nz

    dma = lambda *n: pltpu.SemaphoreType.DMA(n)
    vmem = pl.BlockSpec(memory_space=pltpu.VMEM)
    smem = pl.BlockSpec(memory_space=pltpu.SMEM)
    hbm = pl.BlockSpec(memory_space=pltpu.HBM)
    d_nodes, gathered = pl.pallas_call(
        functools.partial(main_kernel, nr, nc, relations, cap),
        out_shape=(
            jax.ShapeDtypeStruct((nd, f), BF16),
            jax.ShapeDtypeStruct((relations * f, f), BF16),
        ),
        in_specs=[vmem, vmem, smem, smem, smem, vmem, vmem, hbm, hbm],
        out_specs=(hbm, hbm),
        scratch_shapes=[
            pltpu.VMEM((nd, f), BF16),
            pltpu.VMEM((relations * f, f), BF16),
            pltpu.VMEM((f, tn), BF16),
            pltpu.VMEM((tn, f), BF16),
            pltpu.VMEM(weights.shape, BF16),
            pltpu.VMEM((slots, tile, tile), BF16),
            pltpu.VMEM((slots, tile, tile), BF16),
            pltpu.VMEM((nc, nd, f), BF16),
            pltpu.VMEM((relations * nt, nd, f), BF16),
            pltpu.VMEM((slots + 1, nd, f), F32),
            pltpu.VMEM((nk, nd, f), F32),
            pltpu.VMEM((nk, nd, f), F32),
            pltpu.VMEM((nk, nd, f), F32),
            pltpu.VMEM((16, 128), jnp.int32),
            pltpu.SMEM((16, 128), jnp.int32),
            pltpu.VMEM((2, 2, hop, 2 * q, f), BF16),
            pltpu.VMEM((2, 2, hop, 2 * q, f), BF16),
            pltpu.VMEM((2, 2, hop, q, f), BF16),
            pltpu.VMEM((2, 2, hop, q, f), BF16),
            pltpu.VMEM((nz, 2 * q, f), BF16),
            pltpu.VMEM((nz, 2 * q, f), BF16),
            pltpu.VMEM((2, 2 * q, f), BF16),
            pltpu.VMEM((relations, hb, nd, f), F32),
            pltpu.VMEM((relations, f, half), BF16),
            pltpu.VMEM((relations, nr - 1, prow, half), BF16),
            pltpu.VMEM((relations, prow, half), BF16),
            pltpu.VMEM((relations, nk, zrows, 128), BF16),
            dma(4 + relations), dma(SEMS), dma(SEMS),
        ],
        compiler_params=pltpu.CompilerParams(
            collective_id=0, has_side_effects=True, vmem_limit_bytes=67043328
        ),
    )(
        out_grad.T, node_in, tile_rows, tile_cols, tile_count.reshape(relations), tile_rows, tile_cols,
        weights, tile_vals.reshape(slots, tile, tile),
    )
    d_nodes, d_weights = widen(d_nodes, gathered)
    return d_nodes, d_weights.reshape(relations, f, f)


def solution(mesh):
    return jax.shard_map(
        functools.partial(body, mesh.shape["row"], mesh.shape["col"]),
        mesh=mesh,
        in_specs=(
            P("col", "row"),
            P(("row", "col"), None),
            P(),
            P(None, "col", "row", None, None, None),
            P(None, "col", "row", None),
            P(None, "col", "row", None),
            P(None, "col", "row"),
        ),
        out_specs=(P(("row", "col"), None), P()),
        check_vma=False,
    )
```
